32 devices in a mesh: batch: 16 (over z, y, core), rep: 2 (over x).
Axes of the slice: x: 2, y: 2, z: 4, core: 2. Of those that a mesh axis runs over, the one named last changes fastest.
Arguments:
- queries: bfloat16 [2048, 512], P('batch', 'rep'), may hold values from -8 to 8
- passages: bfloat16 [2048, 512], P('batch', 'rep'), may hold values from -8 to 8
- positives: int32 [2048], replicated, may hold values from 0 to 2047, each once
Outputs:
- grad_queries: float32 [2048, 512], P('batch', 'rep')
- grad_passages: float32 [2048, 512], P('batch', 'rep')
The draws below stay inside these ranges and needn't reach their ends.
Inputs may be any that keep to these rules, and one draw needn't show every extreme that they name: `positives`: each passage is the positive of exactly one query.
All inputs are finite; a program needn't handle non-finite values.
Results may differ from the reference program's by a relative error of at most 0.0013.
Values may be sent and summed in bfloat16 or wider, within the bound.
No kernel may reach another device: no remote copies, remote signals or barrier semaphores. Data moves between devices by JAX's collectives and lax.ppermute only.
A program may use at most 128 MiB of HBM per device.

```python
import math
import jax
import jax.numpy as jnp
from jax import lax

D = 512
TOTAL = 2048


def embedding_draw(key, member):
    member_key = jax.random.fold_in(key, member + 11)
    scale_key, entry_key = jax.random.split(member_key, 2)
    row_scale = jnp.exp(jax.random.uniform(scale_key, (TOTAL, 1), jnp.float32, math.log(0.3), math.log(3.0)))
    entries = jax.random.normal(entry_key, (TOTAL, D), jnp.float32)
    values = jnp.clip(row_scale * entries, -8.0, 8.0)
    return values.astype(jnp.bfloat16)


def draw_queries(key, part):
    return embedding_draw(key, 0)


def draw_passages(key, part):
    return embedding_draw(key, 1)


def setup_inputs(seed: int = 0) -> dict:
    key_list = jax.random.split(jax.random.key(seed), 4)
    return {
        "queries": draw_queries(jax.random.fold_in(key_list[3], 71), 0),
        "passages": draw_passages(jax.random.fold_in(key_list[3], 71), 0),
        "positives": jax.random.permutation(key_list[2], TOTAL).astype(jnp.int32),
    }


def block_scores(query_block, passages, logit_scale):
    return jnp.dot(query_block, passages.T, preferred_element_type=jnp.float32) * logit_scale

def reference(queries, passages, positives):
    logit_scale = 1.0 / math.sqrt(D)
    block_rows = math.gcd(TOTAL, 512)
    block_count = TOTAL // block_rows
    query_blocks = queries.reshape(block_count, block_rows, D)
    positive_blocks = positives.reshape(block_count, block_rows)

    def first_sweep(running, query_block):
        column_high, column_total = running
        scores = block_scores(query_block, passages, logit_scale)
        row_high = lax.optimization_barrier(jnp.max(scores, axis=1))
        row_norm = row_high + jnp.log(lax.optimization_barrier(jnp.sum(jnp.exp(scores - row_high[:, None]), axis=1)))
        new_high = jnp.maximum(column_high, lax.optimization_barrier(jnp.max(scores, axis=0)))
        column_total = column_total * jnp.exp(column_high - new_high) + lax.optimization_barrier(jnp.sum(jnp.exp(scores - new_high[None, :]), axis=0))
        return ((new_high, column_total), row_norm)
    starting = (jnp.full((TOTAL,), -1e+30, jnp.float32), jnp.zeros((TOTAL,), jnp.float32))
    (column_high, column_total), row_norms = lax.scan(first_sweep, starting, query_blocks)
    column_norms = column_high + jnp.log(column_total)
    passage_ids = jnp.arange(TOTAL, dtype=jnp.int32)

    def second_sweep(grad_passages, inputs):
        query_block, row_block, positive_block = inputs
        scores = block_scores(query_block, passages, logit_scale)
        matches = (positive_block[:, None] == passage_ids[None, :]).astype(jnp.float32)
        weights = jnp.exp(scores - row_block[:, None]) + jnp.exp(scores - column_norms[None, :]) - 2.0 * matches
        weights = weights.astype(jnp.bfloat16)
        grad_block = jnp.dot(weights, passages, preferred_element_type=jnp.float32) * logit_scale
        grad_passages = grad_passages + jnp.dot(weights.T, query_block, preferred_element_type=jnp.float32) * logit_scale
        return (grad_passages, grad_block)
    grad_passages, grad_blocks = lax.scan(second_sweep, jnp.zeros((TOTAL, D), jnp.float32), (query_blocks, row_norms, positive_blocks))
    return (grad_blocks.reshape(TOTAL, D), grad_passages)
```

```python
import math

import jax
import jax.numpy as jnp
from jax import lax
from jax.experimental import pallas as pl
from jax.experimental.pallas import tpu as pltpu
from jax.sharding import PartitionSpec as P

NEGATIVE = -1e30
LOG2E = 1.4426950408889634
VMEM_BYTES = 58 * 2**20


def joined(x, axis, combine):
    everything = jax.tree.map(lambda part: lax.all_gather(part, axis), x)
    first = jax.tree.map(lambda part: part[0], everything)

    def turn(k, so_far):
        return combine(so_far, jax.tree.map(lambda part: part[k], everything))

    return lax.fori_loop(1, lax.axis_size(axis), turn, first)


def sweep_blocks(update, running, members, offset):
    piece_rows = members[0].shape[0]
    if piece_rows > 1024 and piece_rows % 512 == 0:

        def advance(carried, block_index):
            sliced = tuple(
                (lax.dynamic_slice_in_dim(member, block_index * 512, 512, 0) for member in members)
            )
            return (update(carried, sliced, offset + block_index * 512), None)

        running, unused = lax.scan(advance, running, jnp.arange(piece_rows // 512, dtype=jnp.int32))
        return running
    return update(running, members, offset)


def combine_pairs(former, latter):
    results = []
    for position in range(0, len(former), 2):
        highest = jnp.maximum(former[position], latter[position])
        summed = former[position + 1] * jnp.exp(former[position] - highest) + latter[
            position + 1
        ] * jnp.exp(latter[position] - highest)
        results.extend([highest, summed])
    return tuple(results)


def pair_scores(local_set, remote_set, logit_scale):
    products = lax.dot_general(
        local_set, remote_set, (((1,), (1,)), ((), ())), preferred_element_type=jnp.float32
    )
    return products * logit_scale


def weighted_sum(
    local_set, local_norm, local_keys, remote_set, remote_norm, remote_keys, logit_scale
):
    scores = pair_scores(local_set, remote_set, logit_scale)
    matches = (local_keys[:, None] == remote_keys[None, :]).astype(jnp.float32)
    weights = (
        jnp.exp(scores - local_norm[:, None])
        + jnp.exp(scores - remote_norm[None, :])
        - 2.0 * matches
    )
    return jnp.dot(weights.astype(jnp.bfloat16), remote_set, preferred_element_type=jnp.float32)


def streamed(queries, passages, positives):
    own_rows = queries.shape[0]
    half_rows = own_rows // 2
    model_width = queries.shape[1] * lax.axis_size("rep")
    batch_count = lax.axis_size("batch")
    all_rows = batch_count * own_rows
    column_count = batch_count * half_rows
    logit_scale = 1.0 / math.sqrt(model_width)
    batch_index = lax.axis_index("batch")
    rep_index = lax.axis_index("rep")
    block_start = batch_index * own_rows
    half_start = rep_index * half_rows
    query_full, passage_full = (
        lax.all_gather(queries, "rep", axis=1, tiled=True),
        lax.all_gather(passages, "rep", axis=1, tiled=True),
    )
    passage_half = lax.dynamic_slice_in_dim(passage_full, half_start, half_rows, 0)

    def score_update(running, sliced, offset):
        row_high, row_total, column_high, column_total = running
        scores = pair_scores(query_full, sliced[0], logit_scale)
        new_high = jnp.maximum(row_high, jnp.max(scores, axis=1))
        row_total = row_total * jnp.exp(row_high - new_high) + jnp.sum(
            jnp.exp(scores - new_high[:, None]), axis=1
        )
        piece_high = jnp.max(scores, axis=0)
        piece_total = jnp.sum(jnp.exp(scores - piece_high[None, :]), axis=0)
        column_high = lax.dynamic_update_slice_in_dim(column_high, piece_high, offset, 0)
        column_total = lax.dynamic_update_slice_in_dim(column_total, piece_total, offset, 0)
        return (new_high, row_total, column_high, column_total)

    starting = (
        jnp.full((own_rows,), NEGATIVE, jnp.float32),
        jnp.zeros((own_rows,), jnp.float32),
        jnp.full((column_count,), NEGATIVE, jnp.float32),
        jnp.zeros((column_count,), jnp.float32),
    )
    row_high, row_total, column_high, column_total = sweep_blocks(
        score_update,
        starting,
        (lax.all_gather(passage_half, "batch", axis=0, tiled=True),),
        jnp.int32(0),
    )
    row_high, row_total = joined((row_high, row_total), "rep", combine_pairs)
    column_high, column_total = joined((column_high, column_total), "batch", combine_pairs)
    row_norms = lax.all_gather(row_high + jnp.log(row_total), "batch", axis=0, tiled=True)
    column_halves = lax.all_gather(column_high + jnp.log(column_total), "rep", axis=0, tiled=True)
    column_norms = (
        column_halves.reshape(2, batch_count, half_rows).transpose(1, 0, 2).reshape(all_rows)
    )
    row_own = lax.dynamic_slice_in_dim(row_norms, block_start, own_rows, 0)
    column_own = lax.dynamic_slice_in_dim(column_norms, block_start, own_rows, 0)
    positive_own = lax.dynamic_slice_in_dim(positives, block_start, own_rows, 0)
    own_ids = block_start + jnp.arange(own_rows, dtype=jnp.int32)
    all_ids = jnp.arange(all_rows, dtype=jnp.int32)
    cleared = jnp.zeros((own_rows, model_width), jnp.float32)

    def half_order(vector):
        return lax.dynamic_slice_in_dim(
            vector.reshape(batch_count, own_rows), half_start, half_rows, 1
        ).reshape(column_count)

    column_order = half_order(column_norms)
    row_order = half_order(row_norms)
    positive_order = half_order(positives)
    passage_order = half_order(all_ids)
    query_half = lax.dynamic_slice_in_dim(query_full, half_start, half_rows, 0)

    def both_update(running, sliced, offset):
        query_sum, passage_sum = running
        passage_piece, query_piece = sliced
        piece_rows = passage_piece.shape[0]

        def window(vector):
            return lax.dynamic_slice_in_dim(vector, offset, piece_rows, 0)

        query_sum = query_sum + weighted_sum(
            query_full,
            row_own,
            positive_own,
            passage_piece,
            window(column_order),
            window(passage_order),
            logit_scale,
        )
        passage_sum = passage_sum + weighted_sum(
            passage_full,
            column_own,
            own_ids,
            query_piece,
            window(row_order),
            window(positive_order),
            logit_scale,
        )
        return (query_sum, passage_sum)

    query_sum, passage_sum = sweep_blocks(
        both_update,
        (cleared, cleared),
        (
            lax.all_gather(passage_half, "batch", axis=0, tiled=True),
            lax.all_gather(query_half, "batch", axis=0, tiled=True),
        ),
        jnp.int32(0),
    )
    grad_queries, grad_passages = (
        lax.psum_scatter(query_sum * logit_scale, "rep", scatter_dimension=1, tiled=True),
        lax.psum_scatter(passage_sum * logit_scale, "rep", scatter_dimension=1, tiled=True),
    )
    return (grad_queries, grad_passages)


def exchanged(x, bits):
    axes = ("batch", "rep")
    count = lax.axis_size("batch") * lax.axis_size("rep")
    return lax.ppermute(x, axes, [(i, i ^ bits) for i in range(count)])


def lanes_of(column):
    rows = column.shape[0]
    wide = jnp.broadcast_to(column, (rows, 128))
    parts = [wide[k : k + 128].T[:1] for k in range(0, rows, 128)]
    return jnp.concatenate(parts, axis=1)


def column_of(row):
    return jnp.broadcast_to(row, (128, 128)).T[:, :1]


def matmul(a, b, contract):
    return lax.dot_general(a, b, ((contract[:1], contract[1:]), ((), ())), preferred_element_type=jnp.float32)


def make_stats_kernel(slots, rows, half, scale):
    own_count = slots // 2 * rows
    piece = 256
    pieces = slots * rows // piece
    factor = scale * LOG2E

    def kernel(*refs):
        parts, out, q_all, p_all, scores, row_high = refs[: 2 * slots], *refs[2 * slots :]
        for side in range(2):
            lanes = pl.ds(side * half, half)
            for s in range(slots):
                ref = parts[side * slots + s]
                p_all[pl.ds(s * rows, rows), lanes] = ref[rows:, :]
                if s % 2 == 0:
                    q_all[pl.ds(s // 2 * rows, rows), lanes] = ref[:rows, :]
        row_high[...] = jnp.full((own_count, 128), NEGATIVE, jnp.float32)

        def sweep(j, carry):
            s = matmul(q_all[...], p_all[pl.ds(j * piece, piece), :], (1, 1))
            scores[j] = s
            high = jnp.max(s, axis=0, keepdims=True)
            total = jnp.sum(jnp.exp2((s - high) * factor), axis=0, keepdims=True)
            high = high * scale
            for k in range(piece // 128):
                cut = slice(k * 128, (k + 1) * 128)
                out[pl.ds(slots + j * (piece // 128) + k, 1), :] = high[:, cut]
                out[pl.ds(2 * slots + j * (piece // 128) + k, 1), :] = total[:, cut]
                row_high[...] = jnp.maximum(row_high[...], s[:, cut])
            return carry

        lax.fori_loop(0, pieces, sweep, 0)
        high = jnp.max(row_high[...], axis=1, keepdims=True)

        def add(j, total):
            e = jnp.exp2((scores[j] - high) * factor)
            for k in range(piece // 128):
                total = total + e[:, k * 128 : (k + 1) * 128]
            return total

        total = lax.fori_loop(0, pieces, add, jnp.zeros((own_count, 128), jnp.float32))
        norm = high * scale + jnp.log(jnp.sum(total, axis=1, keepdims=True))
        lanes = lanes_of(norm)
        for k in range(slots // 2):
            out[pl.ds(k, 1), :] = lanes[:, k * 128 : (k + 1) * 128]
            out[pl.ds(slots // 2 + k, 1), :] = lanes[:, k * 128 : (k + 1) * 128]

    return kernel


def make_gradient_kernel(slots, rows, half, scale):
    def kernel(index, *refs):
        parts, (stats, other, positives, query_out, passage_out) = refs[: 2 * slots], refs[2 * slots :]
        block = index[0]

        def joined_set(first):
            return [
                jnp.concatenate([parts[side * slots + s][first : first + rows, :] for s in range(slots)], axis=0)
                for side in range(2)
            ]

        query_sides, passage_sides = joined_set(0), joined_set(rows)
        row_norm, column_norm = [], []
        for s in range(slots):
            t = s ^ 1
            source = stats if s % 2 == 0 else other
            row_norm.append(source[s // 2 : s // 2 + 1, :])
            high, high_other = stats[slots + s : slots + s + 1, :], other[slots + t : slots + t + 1, :]
            total, total_other = stats[2 * slots + s : 2 * slots + s + 1, :], other[2 * slots + t : 2 * slots + t + 1, :]
            top = jnp.maximum(high, high_other)
            summed = total * jnp.exp(high - top) + total_other * jnp.exp(high_other - top)
            column_norm.append(top + jnp.log(summed))
        row_own, column_own = column_of(row_norm[0]), column_of(column_norm[0])
        lane = lax.broadcasted_iota(jnp.int32, (1, rows), 1)
        positive = [positives[pl.ds(block ^ s, 1), :] for s in range(slots)]
        own_id = block * rows + lax.broadcasted_iota(jnp.int32, (rows, 1), 0)
        ids = jnp.concatenate([(block ^ s) * rows + lane for s in range(slots)], axis=1)
        positive_own = column_of(positive[0].astype(jnp.float32)).astype(jnp.int32)

        def gradient(own_sides, all_sides, own_norm, all_norm, own_key, all_key):
            s = matmul(own_sides[0][:rows], all_sides[0], (1, 1)) + matmul(own_sides[1][:rows], all_sides[1], (1, 1))
            s = s * scale
            weights = jnp.exp(s - own_norm) + jnp.exp(s - all_norm) - jnp.where(own_key == all_key, 2.0, 0.0)
            return matmul(weights.astype(jnp.bfloat16), all_sides[0], (1, 0)) * scale

        row_all, column_all = jnp.concatenate(row_norm, axis=1), jnp.concatenate(column_norm, axis=1)
        query_out[...] = gradient(query_sides, passage_sides, row_own, column_all, positive_own, ids)
        passage_out[...] = gradient(
            passage_sides, query_sides, column_own, row_all, own_id, jnp.concatenate(positive, axis=1)
        )

    return kernel


def resident(queries, passages, positives):
    rows, half = queries.shape
    slots, across = lax.axis_size("batch"), lax.axis_size("rep")
    scale = 1.0 / math.sqrt(half * across)
    core, near = across, 2 * across
    unit = jnp.concatenate([queries, passages], axis=0)
    held = {0: unit}
    for k in range(4, slots, 4):
        held[k] = exchanged(unit, k * across)
    sides = [{}, {}]
    for k in range(0, slots, 4):
        sides[0][k] = held[k]
        sides[0][k + 2] = exchanged(held[k], near)
        sides[1][k] = exchanged(held[k], 1)
        sides[1][k + 2] = exchanged(held[k], near + 1)
    for side in sides:
        for k in range(0, slots, 2):
            side[k + 1] = exchanged(side[k], core)
    parts = [side[s] for side in sides for s in range(slots)]
    vmem = pl.BlockSpec(memory_space=pltpu.VMEM)
    params = pltpu.CompilerParams(vmem_limit_bytes=VMEM_BYTES)
    own = slots // 2 * rows
    stats = pl.pallas_call(
        make_stats_kernel(slots, rows, half, scale),
        out_shape=jax.ShapeDtypeStruct((3 * slots, 128), jnp.float32),
        in_specs=[vmem] * len(parts),
        out_specs=vmem,
        scratch_shapes=[
            pltpu.VMEM((own, 2 * half), jnp.bfloat16),
            pltpu.VMEM((slots * rows, 2 * half), jnp.bfloat16),
            pltpu.VMEM((slots * rows // 256, own, 256), jnp.float32),
            pltpu.VMEM((own, 128), jnp.float32),
        ],
        compiler_params=params,
        name="stats",
    )(*parts)
    other = exchanged(stats, core)
    shape = jax.ShapeDtypeStruct((rows, half), jnp.float32)
    return pl.pallas_call(
        make_gradient_kernel(slots, rows, half, scale),
        out_shape=(shape, shape),
        in_specs=[pl.BlockSpec(memory_space=pltpu.SMEM)] + [vmem] * (len(parts) + 3),
        out_specs=(vmem, vmem),
        compiler_params=params,
        name="gradients",
    )(lax.axis_index("batch")[None], *parts, stats, other, positives.reshape(slots, rows))


def fits(rows, half, slots, across):
    everything = slots * rows
    if rows != 128 or half % 128 or across != 2 or slots % 4 or slots & (slots - 1):
        return False
    return everything * half * 16 + everything * everything * 2 <= VMEM_BYTES // 2


def local(queries, passages, positives):
    shape = (*queries.shape, lax.axis_size("batch"), lax.axis_size("rep"))
    return (resident if fits(*shape) else streamed)(queries, passages, positives)


def solution(mesh):
    in_specs = (P("batch", "rep"), P("batch", "rep"), P())
    out_specs = (P("batch", "rep"), P("batch", "rep"))
    return jax.shard_map(local, mesh=mesh, in_specs=in_specs, out_specs=out_specs, check_vma=False)
```

```python
import math

import jax
import jax.numpy as jnp
from jax import lax
from jax.experimental import pallas as pl
from jax.experimental.pallas import tpu as pltpu
from jax.sharding import PartitionSpec as P

NEGATIVE = -1e30
LOG2E = 1.4426950408889634
VMEM_BYTES = 58 * 2**20


def joined(x, axis, combine):
    everything = jax.tree.map(lambda part: lax.all_gather(part, axis), x)
    first = jax.tree.map(lambda part: part[0], everything)

    def turn(k, so_far):
        return combine(so_far, jax.tree.map(lambda part: part[k], everything))

    return lax.fori_loop(1, lax.axis_size(axis), turn, first)


def sweep_blocks(update, running, members, offset):
    piece_rows = members[0].shape[0]
    if piece_rows > 1024 and piece_rows % 512 == 0:

        def advance(carried, block_index):
            sliced = tuple(
                (lax.dynamic_slice_in_dim(member, block_index * 512, 512, 0) for member in members)
            )
            return (update(carried, sliced, offset + block_index * 512), None)

        running, unused = lax.scan(advance, running, jnp.arange(piece_rows // 512, dtype=jnp.int32))
        return running
    return update(running, members, offset)


def combine_pairs(former, latter):
    results = []
    for position in range(0, len(former), 2):
        highest = jnp.maximum(former[position], latter[position])
        summed = former[position + 1] * jnp.exp(former[position] - highest) + latter[
            position + 1
        ] * jnp.exp(latter[position] - highest)
        results.extend([highest, summed])
    return tuple(results)


def pair_scores(local_set, remote_set, logit_scale):
    products = lax.dot_general(
        local_set, remote_set, (((1,), (1,)), ((), ())), preferred_element_type=jnp.float32
    )
    return products * logit_scale


def weighted_sum(
    local_set, local_norm, local_keys, remote_set, remote_norm, remote_keys, logit_scale
):
    scores = pair_scores(local_set, remote_set, logit_scale)
    matches = (local_keys[:, None] == remote_keys[None, :]).astype(jnp.float32)
    weights = (
        jnp.exp(scores - local_norm[:, None])
        + jnp.exp(scores - remote_norm[None, :])
        - 2.0 * matches
    )
    return jnp.dot(weights.astype(jnp.bfloat16), remote_set, preferred_element_type=jnp.float32)


def streamed(queries, passages, positives):
    own_rows = queries.shape[0]
    half_rows = own_rows // 2
    model_width = queries.shape[1] * lax.axis_size("rep")
    batch_count = lax.axis_size("batch")
    all_rows = batch_count * own_rows
    column_count = batch_count * half_rows
    logit_scale = 1.0 / math.sqrt(model_width)
    batch_index = lax.axis_index("batch")
    rep_index = lax.axis_index("rep")
    block_start = batch_index * own_rows
    half_start = rep_index * half_rows
    query_full, passage_full = (
        lax.all_gather(queries, "rep", axis=1, tiled=True),
        lax.all_gather(passages, "rep", axis=1, tiled=True),
    )
    passage_half = lax.dynamic_slice_in_dim(passage_full, half_start, half_rows, 0)

    def score_update(running, sliced, offset):
        row_high, row_total, column_high, column_total = running
        scores = pair_scores(query_full, sliced[0], logit_scale)
        new_high = jnp.maximum(row_high, jnp.max(scores, axis=1))
        row_total = row_total * jnp.exp(row_high - new_high) + jnp.sum(
            jnp.exp(scores - new_high[:, None]), axis=1
        )
        piece_high = jnp.max(scores, axis=0)
        piece_total = jnp.sum(jnp.exp(scores - piece_high[None, :]), axis=0)
        column_high = lax.dynamic_update_slice_in_dim(column_high, piece_high, offset, 0)
        column_total = lax.dynamic_update_slice_in_dim(column_total, piece_total, offset, 0)
        return (new_high, row_total, column_high, column_total)

    starting = (
        jnp.full((own_rows,), NEGATIVE, jnp.float32),
        jnp.zeros((own_rows,), jnp.float32),
        jnp.full((column_count,), NEGATIVE, jnp.float32),
        jnp.zeros((column_count,), jnp.float32),
    )
    row_high, row_total, column_high, column_total = sweep_blocks(
        score_update,
        starting,
        (lax.all_gather(passage_half, "batch", axis=0, tiled=True),),
        jnp.int32(0),
    )
    row_high, row_total = joined((row_high, row_total), "rep", combine_pairs)
    column_high, column_total = joined((column_high, column_total), "batch", combine_pairs)
    row_norms = lax.all_gather(row_high + jnp.log(row_total), "batch", axis=0, tiled=True)
    column_halves = lax.all_gather(column_high + jnp.log(column_total), "rep", axis=0, tiled=True)
    column_norms = (
        column_halves.reshape(2, batch_count, half_rows).transpose(1, 0, 2).reshape(all_rows)
    )
    row_own = lax.dynamic_slice_in_dim(row_norms, block_start, own_rows, 0)
    column_own = lax.dynamic_slice_in_dim(column_norms, block_start, own_rows, 0)
    positive_own = lax.dynamic_slice_in_dim(positives, block_start, own_rows, 0)
    own_ids = block_start + jnp.arange(own_rows, dtype=jnp.int32)
    all_ids = jnp.arange(all_rows, dtype=jnp.int32)
    cleared = jnp.zeros((own_rows, model_width), jnp.float32)

    def half_order(vector):
        return lax.dynamic_slice_in_dim(
            vector.reshape(batch_count, own_rows), half_start, half_rows, 1
        ).reshape(column_count)

    column_order = half_order(column_norms)
    row_order = half_order(row_norms)
    positive_order = half_order(positives)
    passage_order = half_order(all_ids)
    query_half = lax.dynamic_slice_in_dim(query_full, half_start, half_rows, 0)

    def both_update(running, sliced, offset):
        query_sum, passage_sum = running
        passage_piece, query_piece = sliced
        piece_rows = passage_piece.shape[0]

        def window(vector):
            return lax.dynamic_slice_in_dim(vector, offset, piece_rows, 0)

        query_sum = query_sum + weighted_sum(
            query_full,
            row_own,
            positive_own,
            passage_piece,
            window(column_order),
            window(passage_order),
            logit_scale,
        )
        passage_sum = passage_sum + weighted_sum(
            passage_full,
            column_own,
            own_ids,
            query_piece,
            window(row_order),
            window(positive_order),
            logit_scale,
        )
        return (query_sum, passage_sum)

    query_sum, passage_sum = sweep_blocks(
        both_update,
        (cleared, cleared),
        (
            lax.all_gather(passage_half, "batch", axis=0, tiled=True),
            lax.all_gather(query_half, "batch", axis=0, tiled=True),
        ),
        jnp.int32(0),
    )
    grad_queries, grad_passages = (
        lax.psum_scatter(query_sum * logit_scale, "rep", scatter_dimension=1, tiled=True),
        lax.psum_scatter(passage_sum * logit_scale, "rep", scatter_dimension=1, tiled=True),
    )
    return (grad_queries, grad_passages)


def exchanged(x, bits):
    axes = ("batch", "rep")
    count = lax.axis_size("batch") * lax.axis_size("rep")
    return lax.ppermute(x, axes, [(i, i ^ bits) for i in range(count)])


def lanes_of(column):
    rows = column.shape[0]
    wide = jnp.broadcast_to(column, (rows, 128))
    parts = [wide[k : k + 128].T[:1] for k in range(0, rows, 128)]
    return jnp.concatenate(parts, axis=1)


def column_of(row):
    return jnp.broadcast_to(row, (128, 128)).T[:, :1]


def matmul(a, b, contract):
    return lax.dot_general(a, b, ((contract[:1], contract[1:]), ((), ())), preferred_element_type=jnp.float32)


def make_pack_kernel(rows, half):
    def kernel(*refs):
        parts, query_out, passage_out = refs[:-2], refs[-2], refs[-1]
        count = len(parts) // 2
        for side in range(2):
            lanes = pl.ds(side * half, half)
            for s in range(count):
                query_out[pl.ds(s * rows, rows), lanes] = parts[side * count + s][:rows, :]
                passage_out[pl.ds(s * rows, rows), lanes] = parts[side * count + s][rows:, :]

    return kernel


def make_stats_kernel(scale, last):
    piece = 256
    factor = scale * LOG2E

    def kernel(*refs):
        queries, passages = refs[:2]
        if last:
            high_in, total_in, column_in, out, scores = refs[2:]
        else:
            high_out, total_out, column_out, scores = refs[2:]
        count = passages.shape[0] // piece
        lead = passages.shape[0] // 128
        near = queries.shape[0] // 128
        row_high = None
        for j in range(count):
            s = matmul(queries[...], passages[j * piece : (j + 1) * piece, :], (1, 1))
            scores[j] = s
            high = jnp.max(s, axis=0, keepdims=True)
            total = jnp.sum(jnp.exp2((s - high) * factor), axis=0, keepdims=True)
            high = high * scale
            wide = s[:, :128]
            for k in range(piece // 128):
                cut = slice(k * 128, (k + 1) * 128)
                row = j * (piece // 128) + k
                if last:
                    out[near + lead + row : near + lead + row + 1, :] = high[:, cut]
                    out[near + 3 * lead + row : near + 3 * lead + row + 1, :] = total[:, cut]
                else:
                    column_out[row : row + 1, :] = high[:, cut]
                    column_out[lead + row : lead + row + 1, :] = total[:, cut]
                wide = jnp.maximum(wide, s[:, cut])
            row_high = wide if row_high is None else jnp.maximum(row_high, wide)
        high = jnp.max(row_high, axis=1, keepdims=True)
        sums = jnp.zeros(row_high.shape, jnp.float32)
        for j in range(count):
            e = jnp.exp2((scores[j] - high) * factor)
            for k in range(piece // 128):
                sums = sums + e[:, k * 128 : (k + 1) * 128]
        if last:
            top = jnp.maximum(high, high_in[...])
            sums = sums * jnp.exp2((high - top) * factor) + total_in[...] * jnp.exp2((high_in[...] - top) * factor)
            norm = top[:, :1] * scale + jnp.log(jnp.sum(sums, axis=1, keepdims=True))
            lanes = lanes_of(norm)
            for k in range(near):
                out[k : k + 1, :] = lanes[:, k * 128 : (k + 1) * 128]
            out[near : near + lead, :] = column_in[:lead, :]
            out[near + 2 * lead : near + 3 * lead, :] = column_in[lead:, :]
        else:
            high_out[...] = jnp.broadcast_to(high, row_high.shape)
            total_out[...] = sums

    return kernel


def make_gradient_kernel(slots, rows, half, scale):
    near = slots // 2
    piece = 512

    def kernel(index, own_q, own_p, far_q, far_p, mine, theirs, positives, query_out, passage_out):
        block = index[0]
        lane = lax.broadcasted_iota(jnp.int32, (1, rows), 1)
        row_norm = [mine[s : s + 1, :] for s in range(near)] + [theirs[s : s + 1, :] for s in range(near)]
        column_norm, ids, positive = [], [], []
        for s in range(slots):
            c, t = near + s, near + (s + near) % slots
            high, high_far = mine[c : c + 1, :], theirs[t : t + 1, :]
            total, total_far = mine[c + slots : c + slots + 1, :], theirs[t + slots : t + slots + 1, :]
            top = jnp.maximum(high, high_far)
            summed = total * jnp.exp(high - top) + total_far * jnp.exp(high_far - top)
            column_norm.append(top + jnp.log(summed))
            other = block ^ (s % near * 2 + s // near)
            ids.append(other * rows + lane)
            positive.append(positives[pl.ds(other, 1), :])
        row_own, column_own = column_of(row_norm[0]), column_of(column_norm[0])
        own_id = block * rows + lax.broadcasted_iota(jnp.int32, (rows, 1), 0)
        positive_own = column_of(positive[0].astype(jnp.float32)).astype(jnp.int32)

        def gradient(own, everything, own_norm, norms, own_key, keys):
            result = jnp.zeros((rows, half), jnp.float32)
            for start in range(0, slots * rows, piece):
                source = everything[start // (near * rows)]
                local_rows = pl.ds(start % (near * rows), piece)
                cut = slice(start // rows, (start + piece) // rows)
                s = matmul(own, source[local_rows, :], (1, 1)) * scale
                norm, key = jnp.concatenate(norms[cut], axis=1), jnp.concatenate(keys[cut], axis=1)
                weights = jnp.exp(s - own_norm) + jnp.exp(s - norm) - jnp.where(own_key == key, 2.0, 0.0)
                result = result + matmul(weights.astype(jnp.bfloat16), source[local_rows, :half], (1, 0))
            return result * scale

        query_out[...] = gradient(own_q[:rows, :], (own_p, far_p), row_own, column_norm, positive_own, ids)
        passage_out[...] = gradient(own_p[:rows, :], (own_q, far_q), column_own, row_norm, own_id, positive)

    return kernel


def resident(queries, passages, positives):
    rows, half = queries.shape
    slots, across = lax.axis_size("batch"), lax.axis_size("rep")
    scale = 1.0 / math.sqrt(half * across)
    core, near = across, 2 * across
    unit = jnp.concatenate([queries, passages], axis=0)
    held = {0: unit}
    for k in range(4, slots, 4):
        held[k] = exchanged(unit, k * across)
    sides = [{}, {}]
    for k in range(0, slots, 4):
        sides[0][k] = held[k]
        sides[0][k + 2] = exchanged(held[k], near)
        sides[1][k] = exchanged(held[k], 1)
        sides[1][k + 2] = exchanged(held[k], near + 1)
    parts = [side[s] for side in sides for s in range(0, slots, 2)]
    own = slots // 2 * rows
    vmem = pl.BlockSpec(memory_space=pltpu.VMEM)

    def call(kernel, name, shapes, *args, scratch=()):
        specs = [pl.BlockSpec(memory_space=pltpu.SMEM) if a.size == 1 else vmem for a in args]
        args = [a if a.size == 1 else pltpu.with_memory_space_constraint(a, pltpu.VMEM) for a in args]
        return pl.pallas_call(
            kernel,
            out_shape=shapes,
            in_specs=specs,
            out_specs=tuple(vmem for _ in shapes),
            scratch_shapes=scratch,
            compiler_params=pltpu.CompilerParams(vmem_limit_bytes=VMEM_BYTES // 4),
            name=name,
        )(*args)

    def array(*shape, dtype=jnp.float32):
        return pltpu.VMEM(shape, dtype)

    packed = array(own, half * across, dtype=queries.dtype)
    own_q, own_p = call(make_pack_kernel(rows, half), "pack", (packed, packed), *parts)
    far_p, far_q = exchanged(own_p, core), exchanged(own_q, core)
    columns = array(slots, 128)
    scores = [pltpu.VMEM((own // 256, own, 256), jnp.float32)]
    high, total, first = call(
        make_stats_kernel(scale, False),
        "stats_own",
        (array(own, 128), array(own, 128), columns),
        own_q,
        own_p,
        scratch=scores,
    )
    (mine,) = call(
        make_stats_kernel(scale, True),
        "stats_far",
        (array(5 * slots // 2, 128),),
        own_q,
        far_p,
        high,
        total,
        first,
        scratch=scores,
    )
    shape = jax.ShapeDtypeStruct((rows, half), jnp.float32)
    return call(
        make_gradient_kernel(slots, rows, half, scale),
        "gradients",
        (shape, shape),
        lax.axis_index("batch")[None],
        own_q,
        own_p,
        far_q,
        far_p,
        mine,
        exchanged(mine, core),
        positives.reshape(slots, rows),
    )


def fits(rows, half, slots, across):
    everything = slots * rows
    if rows != 128 or half % 128 or across != 2 or slots % 4 or slots & (slots - 1):
        return False
    return everything * half * 16 + everything * everything * 2 <= VMEM_BYTES // 2


def local(queries, passages, positives):
    shape = (*queries.shape, lax.axis_size("batch"), lax.axis_size("rep"))
    return (resident if fits(*shape) else streamed)(queries, passages, positives)


def solution(mesh):
    in_specs = (P("batch", "rep"), P("batch", "rep"), P())
    out_specs = (P("batch", "rep"), P("batch", "rep"))
    return jax.shard_map(local, mesh=mesh, in_specs=in_specs, out_specs=out_specs, check_vma=False)
```

```python
import math

import jax
import jax.numpy as jnp
from jax import lax
from jax.experimental import pallas as pl
from jax.experimental.pallas import tpu as pltpu
from jax.sharding import PartitionSpec as P


NEGATIVE = -1e30
LOG2E = 1.4426950408889634
VMEM_BYTES = 58 * 2**20
DIAGONAL = "xyxd"
PIECE = 256


def joined(x, axis, combine):
    everything = jax.tree.map(lambda part: lax.all_gather(part, axis), x)
    first = jax.tree.map(lambda part: part[0], everything)

    def turn(k, so_far):
        return combine(so_far, jax.tree.map(lambda part: part[k], everything))

    return lax.fori_loop(1, lax.axis_size(axis), turn, first)


def sweep_blocks(update, running, members, offset):
    piece_rows = members[0].shape[0]
    if piece_rows > 1024 and piece_rows % 512 == 0:

        def advance(carried, block_index):
            sliced = tuple(
                (lax.dynamic_slice_in_dim(member, block_index * 512, 512, 0) for member in members)
            )
            return (update(carried, sliced, offset + block_index * 512), None)

        running, _ = lax.scan(advance, running, jnp.arange(piece_rows // 512, dtype=jnp.int32))
        return running
    return update(running, members, offset)


def combine_pairs(former, latter):
    results = []
    for position in range(0, len(former), 2):
        highest = jnp.maximum(former[position], latter[position])
        summed = former[position + 1] * jnp.exp(former[position] - highest) + latter[
            position + 1
        ] * jnp.exp(latter[position] - highest)
        results.extend([highest, summed])
    return tuple(results)


def pair_scores(local_set, remote_set, logit_scale):
    products = lax.dot_general(
        local_set, remote_set, (((1,), (1,)), ((), ())), preferred_element_type=jnp.float32
    )
    return products * logit_scale


def weighted_sum(
    local_set, local_norm, local_keys, remote_set, remote_norm, remote_keys, logit_scale
):
    scores = pair_scores(local_set, remote_set, logit_scale)
    matches = (local_keys[:, None] == remote_keys[None, :]).astype(jnp.float32)
    weights = (
        jnp.exp(scores - local_norm[:, None])
        + jnp.exp(scores - remote_norm[None, :])
        - 2.0 * matches
    )
    return jnp.dot(weights.astype(jnp.bfloat16), remote_set, preferred_element_type=jnp.float32)


def streamed(queries, passages, positives):
    own_rows = queries.shape[0]
    half_rows = own_rows // 2
    model_width = queries.shape[1] * lax.axis_size("rep")
    batch_count = lax.axis_size("batch")
    all_rows = batch_count * own_rows
    column_count = batch_count * half_rows
    logit_scale = 1.0 / math.sqrt(model_width)
    batch_index = lax.axis_index("batch")
    rep_index = lax.axis_index("rep")
    block_start = batch_index * own_rows
    half_start = rep_index * half_rows
    query_full, passage_full = (
        lax.all_gather(queries, "rep", axis=1, tiled=True),
        lax.all_gather(passages, "rep", axis=1, tiled=True),
    )
    passage_half = lax.dynamic_slice_in_dim(passage_full, half_start, half_rows, 0)

    def score_update(running, sliced, offset):
        row_high, row_total, column_high, column_total = running
        scores = pair_scores(query_full, sliced[0], logit_scale)
        new_high = jnp.maximum(row_high, jnp.max(scores, axis=1))
        row_total = row_total * jnp.exp(row_high - new_high) + jnp.sum(
            jnp.exp(scores - new_high[:, None]), axis=1
        )
        piece_high = jnp.max(scores, axis=0)
        piece_total = jnp.sum(jnp.exp(scores - piece_high[None, :]), axis=0)
        column_high = lax.dynamic_update_slice_in_dim(column_high, piece_high, offset, 0)
        column_total = lax.dynamic_update_slice_in_dim(column_total, piece_total, offset, 0)
        return (new_high, row_total, column_high, column_total)

    starting = (
        jnp.full((own_rows,), NEGATIVE, jnp.float32),
        jnp.zeros((own_rows,), jnp.float32),
        jnp.full((column_count,), NEGATIVE, jnp.float32),
        jnp.zeros((column_count,), jnp.float32),
    )
    row_high, row_total, column_high, column_total = sweep_blocks(
        score_update,
        starting,
        (lax.all_gather(passage_half, "batch", axis=0, tiled=True),),
        jnp.int32(0),
    )
    row_high, row_total = joined((row_high, row_total), "rep", combine_pairs)
    column_high, column_total = joined((column_high, column_total), "batch", combine_pairs)
    row_norms = lax.all_gather(row_high + jnp.log(row_total), "batch", axis=0, tiled=True)
    column_halves = lax.all_gather(column_high + jnp.log(column_total), "rep", axis=0, tiled=True)
    column_norms = (
        column_halves.reshape(2, batch_count, half_rows).transpose(1, 0, 2).reshape(all_rows)
    )
    row_own = lax.dynamic_slice_in_dim(row_norms, block_start, own_rows, 0)
    column_own = lax.dynamic_slice_in_dim(column_norms, block_start, own_rows, 0)
    positive_own = lax.dynamic_slice_in_dim(positives, block_start, own_rows, 0)
    own_ids = block_start + jnp.arange(own_rows, dtype=jnp.int32)
    all_ids = jnp.arange(all_rows, dtype=jnp.int32)
    cleared = jnp.zeros((own_rows, model_width), jnp.float32)

    def half_order(vector):
        return lax.dynamic_slice_in_dim(
            vector.reshape(batch_count, own_rows), half_start, half_rows, 1
        ).reshape(column_count)

    column_order = half_order(column_norms)
    row_order = half_order(row_norms)
    positive_order = half_order(positives)
    passage_order = half_order(all_ids)
    query_half = lax.dynamic_slice_in_dim(query_full, half_start, half_rows, 0)

    def both_update(running, sliced, offset):
        query_sum, passage_sum = running
        passage_piece, query_piece = sliced
        piece_rows = passage_piece.shape[0]

        def window(vector):
            return lax.dynamic_slice_in_dim(vector, offset, piece_rows, 0)

        query_sum = query_sum + weighted_sum(
            query_full,
            row_own,
            positive_own,
            passage_piece,
            window(column_order),
            window(passage_order),
            logit_scale,
        )
        passage_sum = passage_sum + weighted_sum(
            passage_full,
            column_own,
            own_ids,
            query_piece,
            window(row_order),
            window(positive_order),
            logit_scale,
        )
        return (query_sum, passage_sum)

    query_sum, passage_sum = sweep_blocks(
        both_update,
        (cleared, cleared),
        (
            lax.all_gather(passage_half, "batch", axis=0, tiled=True),
            lax.all_gather(query_half, "batch", axis=0, tiled=True),
        ),
        jnp.int32(0),
    )
    grad_queries, grad_passages = (
        lax.psum_scatter(query_sum * logit_scale, "rep", scatter_dimension=1, tiled=True),
        lax.psum_scatter(passage_sum * logit_scale, "rep", scatter_dimension=1, tiled=True),
    )
    return (grad_queries, grad_passages)


def exchanged(x, bits):
    axes = ("batch", "rep")
    count = lax.axis_size("batch") * lax.axis_size("rep")
    return lax.ppermute(x, axes, [(i, i ^ bits) for i in range(count)])


def column_of(row):
    return jnp.broadcast_to(row, (128, 128)).T[:, :1]


def matmul(a, b, contract):
    return lax.dot_general(a, b, ((contract[:1], contract[1:]), ((), ())), preferred_element_type=jnp.float32)


def make_unit_kernel(offsets, rows):
    def kernel(index, queries, passages, positives, unit, keys, table, arrived):
        copies = [
            pltpu.make_async_copy(source, target, arrived.at[n])
            for n, (source, target) in enumerate(
                ((queries, unit.at[:rows]), (passages, unit.at[rows:]), (positives, table))
            )
        ]
        for copy in copies:
            copy.start()
        for copy in copies[::-1]:
            copy.wait()
        lane = lax.broadcasted_iota(jnp.int32, (1, rows), 1)
        for s, offset in enumerate(offsets):
            block = index[0] ^ offset
            keys[s : s + 1, :] = block * rows + lane
            keys[len(offsets) + s : len(offsets) + s + 1, :] = table[pl.ds(block, 1), :]

    return kernel


def make_pack_kernel(rows, half):
    def kernel(*refs):
        parts, query_out, passage_out = refs[:-2], refs[-2], refs[-1]
        count = len(parts) // 2
        for side in range(2):
            lanes = pl.ds(side * half, half)
            for s in range(count):
                query_out[pl.ds(s * rows, rows), lanes] = parts[side * count + s][:rows, :]
                passage_out[pl.ds(s * rows, rows), lanes] = parts[side * count + s][rows:, :]

    return kernel


def joined_stats(blocks, former, factor, fold):
    high = None if former is None else former[0]
    for block in blocks:
        for part in fold(block):
            high = part if high is None else jnp.maximum(high, part)
    sums = None if former is None else former[1] * jnp.exp2((former[0] - high) * factor)
    for block in blocks:
        for part in fold(block):
            more = jnp.exp2((part - high) * factor)
            sums = more if sums is None else sums + more
    return high, sums


def put_turned(out, block):
    for k in range(0, block.shape[0], 128):
        out[:, k : k + 128] = block[k : k + 128].T


def by_lane(block):
    return [block[:, k : k + 128] for k in range(0, block.shape[1], 128)]


def column_stats(blocks, former, factor):
    high = None if former is None else former[0]
    for block in blocks:
        peak = jnp.max(block[...].reshape(-1, 8, block.shape[1]), axis=0)
        high = peak if high is None else jnp.maximum(high, peak)
    sums = None if former is None else former[1] * jnp.exp2((former[0] - high) * factor)
    for block in blocks:
        part = jnp.sum(jnp.exp2((block[...].reshape(-1, 8, block.shape[1]) - high) * factor), axis=0)
        sums = part if sums is None else sums + part
    return high, sums


def make_early_kernel(scale, joins, rows):
    factor = scale * LOG2E

    def kernel(*refs):
        queries, passages = refs[:2]
        high_out, sum_out, column_high, column_sum, kept = refs[-7:-2] if not joins else refs[-6:-1]
        scores = refs[-1]
        count = passages.shape[0] // PIECE
        blocks = [scores.at[j] for j in range(count)]
        for j in range(count):
            cut = slice(j * PIECE, (j + 1) * PIECE)
            s = matmul(queries[...], passages[cut, :], (1, 1))
            blocks[j][...] = s
            kept[:, cut] = s[:rows]
            if j == 0 and not joins:
                put_turned(refs[-2], s[:, :rows])
            column_high[:, cut], column_sum[:, cut] = column_stats([blocks[j]], None, factor)
        former = (refs[2][...], refs[3][...]) if joins else None
        high_out[...], sum_out[...] = joined_stats(blocks, former, factor, by_lane)

    return kernel


def make_late_kernel(scale, last, rows):
    factor = scale * LOG2E

    def kernel(*refs):
        early_q, late_q, early_p, late_p, high_in, sum_in, column_high, column_sum = refs[:8]
        across, corner = refs[-2:]
        kept = refs[-3 if last else -4]
        early, late = early_p.shape[0], late_p.shape[0]
        lead = (early + late) // 128
        pieces = late // PIECE
        tops = [across.at[j] for j in range(pieces)]
        corners = [corner.at[j] for j in range((early + late) // PIECE)]
        columns = []
        for j in range(early // PIECE):
            cut = slice(j * PIECE, (j + 1) * PIECE)
            block = corners[pieces + j]
            s = matmul(late_q[...], early_p[cut, :], (1, 1))
            block[...] = s
            if j == 0 and not last:
                put_turned(refs[-3], s[:, :rows])
            columns.append(column_stats([block], (column_high[:, cut], column_sum[:, cut]), factor))
        for j in range(pieces):
            cut = slice(j * PIECE, (j + 1) * PIECE)
            s = matmul(early_q[...], late_p[cut, :], (1, 1))
            tops[j][...] = s
            kept[:, cut] = s[:rows]
            corners[j][...] = matmul(late_q[...], late_p[cut, :], (1, 1))
            columns.append(column_stats([tops[j], corners[j]], None, factor))
        late_former = (refs[8][...], refs[9][...]) if last else None
        groups = (
            joined_stats(tops, (high_in[...], sum_in[...]), factor, by_lane),
            joined_stats(corners, late_former, factor, by_lane),
        )
        if not last:
            for n, values in enumerate((*groups[0], *groups[1])):
                refs[8 + n][...] = values
            for j, (high, sums) in enumerate(columns):
                cut = slice(j * PIECE, (j + 1) * PIECE)
                refs[12][:, cut], refs[13][:, cut] = high, sums
            return
        out = refs[12]
        near = [(refs[10][:, j : j + PIECE], refs[11][:, j : j + PIECE]) for j in range(0, early + late, PIECE)]
        for side, pairs in enumerate((near, columns)):
            for j, (high, sums) in enumerate(pairs):
                top = jnp.max(high, axis=0, keepdims=True)
                total = jnp.sum(sums * jnp.exp2((high - top) * factor), axis=0, keepdims=True)
                for k in range(PIECE // 128):
                    cut, row = slice(k * 128, (k + 1) * 128), 2 * side * lead + j * (PIECE // 128) + k
                    out[row : row + 1, :] = top[:, cut]
                    out[lead + row : lead + row + 1, :] = total[:, cut]
        row = 4 * lead
        first_half = lax.broadcasted_iota(jnp.int32, (128, 128), 1) < 64
        for high, sums in groups:
            top = jnp.max(high, axis=1, keepdims=True)
            total = jnp.sum(sums * jnp.exp2((high - top) * factor), axis=1, keepdims=True)
            for k in range(0, high.shape[0], 128):
                both = jnp.where(first_half, top[k : k + 128], total[k : k + 128]).T
                out[row : row + 1, :] = both[:1] * scale + jnp.log(both[64:65])
                row += 1

    return kernel


def make_scores_kernel():
    def kernel(own, *refs):
        sources, out = refs[:-1], refs[-1]
        rows = out.shape[0]
        start = 0
        for source in sources:
            for low in range(0, source.shape[0], PIECE):
                out[:, start : start + PIECE] = matmul(own[:rows, :], source[low : low + PIECE, :], (1, 1))
                start += PIECE

    return kernel


def make_gradient_kernel(slots, rows, half, scale):
    near = slots // 2

    def kernel(*refs):
        keys, mine, theirs, query_out, passage_out = refs[-5:]
        queries, passages = refs[:4], refs[4:8]
        scores = refs[8:12], refs[12:15]
        end = 2 * slots
        row_norm = [source[end + s : end + s + 1, :] for source in (mine, theirs) for s in range(near)]
        column_norm = []
        for s in range(slots):
            c = s % near + s // near * slots
            t = (c + slots) % (2 * slots)
            high, high_far = mine[c : c + 1, :], theirs[t : t + 1, :]
            total, total_far = mine[c + near : c + near + 1, :], theirs[t + near : t + near + 1, :]
            top = jnp.maximum(high, high_far)
            summed = total * jnp.exp((high - top) * scale) + total_far * jnp.exp((high_far - top) * scale)
            column_norm.append(top * scale + jnp.log(summed))
        ids = [keys[s : s + 1, :] for s in range(slots)]
        positive = [keys[slots + s : slots + s + 1, :] for s in range(slots)]
        own_id, positive_own = (column_of(k[0].astype(jnp.float32)).astype(jnp.int32) for k in (ids, positive))
        tasks = (
            (scores[0], passages, column_of(row_norm[0]), column_norm, positive_own, ids),
            (scores[1], queries, column_of(column_norm[0]), row_norm, own_id, positive),
        )
        results = [None, None]
        spans = [(n, low) for n, source in enumerate(passages) for low in range(0, source.shape[0], PIECE)]
        for step, (n, low) in enumerate(spans):
            cut = slice(step * PIECE // rows, (step + 1) * PIECE // rows)
            for k, (parts, everything, own_norm, norms, own_key, all_keys) in enumerate(tasks):
                at, start = n, low
                if n >= len(parts) - 1:
                    at = len(parts) - 1
                    start = low + sum(source.shape[0] for source in passages[at:n])
                s = parts[at][:, start : start + PIECE] * scale
                norm, key = jnp.concatenate(norms[cut], axis=1), jnp.concatenate(all_keys[cut], axis=1)
                weights = jnp.exp(s - own_norm) + jnp.exp(s - norm) - jnp.where(own_key == key, 2.0, 0.0)
                part = matmul(weights.astype(jnp.bfloat16), everything[n][low : low + PIECE, :half], (1, 0))
                results[k] = part if results[k] is None else results[k] + part
        query_out[...], passage_out[...] = results[0] * scale, results[1] * scale

    return kernel


def resident(queries, passages, positives):
    rows, half = queries.shape
    slots, across = lax.axis_size("batch"), lax.axis_size("rep")
    scale = 1.0 / math.sqrt(half * across)
    core, near = across, 2 * across
    vmem = pl.BlockSpec(memory_space=pltpu.VMEM)

    def call(kernel, name, shapes, *args, scratch=()):
        specs = [pl.BlockSpec(memory_space=pltpu.SMEM) if a.size == 1 else vmem for a in args]
        if name == "unit":
            specs[1:] = [pl.BlockSpec(memory_space=pl.ANY)] * 3
        space = pltpu.HBM if name == "unit" else pltpu.VMEM
        args = [a if a.size == 1 else pltpu.with_memory_space_constraint(a, space) for a in args]
        return pl.pallas_call(
            kernel,
            out_shape=shapes,
            in_specs=specs,
            out_specs=tuple(vmem for _ in shapes),
            scratch_shapes=scratch,
            compiler_params=pltpu.CompilerParams(vmem_limit_bytes=VMEM_BYTES // 8),
        )(*args)

    def array(*shape, dtype=jnp.float32):
        return pltpu.VMEM(shape, dtype)

    late_slots = [s for s in range(slots // 2, slots, 2) if s & 2]
    early_slots = [s for s in range(0, slots, 2) if s not in late_slots]
    order = early_slots + late_slots
    order += [s ^ 1 for s in order]
    unit, keys = call(
        make_unit_kernel(order, rows),
        "unit",
        (array(2 * rows, half, dtype=queries.dtype), array(2 * slots, 128, dtype=jnp.int32)),
        lax.axis_index("batch")[None],
        queries,
        passages,
        positives.reshape(slots, rows),
        scratch=[pltpu.VMEM((slots, rows), jnp.int32), pltpu.SemaphoreType.DMA((3,))],
    )
    held = {0: unit}
    for k in range(4, slots, 4):
        held[k] = exchanged(unit, k * across)
    sides = [{}, {}]
    for k in range(0, slots, 4):
        n = k // 4
        sides[0][k] = held[k]
        sides[0][k + 2] = exchanged(held[k], near)
        sides[1][k] = exchanged(held[k], 1)
        mode = DIAGONAL[n % len(DIAGONAL)]
        if mode == "d":
            sides[1][k + 2] = exchanged(held[k], near + 1)
        elif mode == "x":
            sides[1][k + 2] = exchanged(sides[1][k], near)
        else:
            sides[1][k + 2] = exchanged(sides[0][k + 2], 1)

    def packed(name, chosen):
        shape = array(len(chosen) * rows, half * across, dtype=queries.dtype)
        parts = [side[s] for side in sides for s in chosen]
        q, p = call(make_pack_kernel(rows, half), "pack_" + name, (shape, shape), *parts)
        far_p, far_q = exchanged(p, core), exchanged(q, core)
        return q, p, far_q, far_p

    early, late = len(early_slots) * rows, len(late_slots) * rows
    early_q, early_p, early_far_q, early_far_p = packed("early", early_slots)
    own = slots // 2 * rows
    columns = (array(8, early), array(8, early))
    row = (array(early, 128), array(early, 128))
    scores = [pltpu.VMEM((early // PIECE, early, PIECE), jnp.float32)]
    high, sums, *columns_near, kept_0, turned_0 = call(
        make_early_kernel(scale, False, rows),
        "early_near",
        (*row, *columns, array(rows, early), array(rows, early)),
        early_q,
        early_p,
        scratch=scores,
    )
    high, sums, *columns_far, kept_2 = call(
        make_early_kernel(scale, True, rows),
        "early_far",
        (*row, *columns, array(rows, early)),
        early_q,
        early_far_p,
        high,
        sums,
        scratch=scores,
    )
    late_q, late_p, late_far_q, late_far_p = packed("late", late_slots)
    late_row = (array(late, 128), array(late, 128))
    scores = [
        pltpu.VMEM((late // PIECE, early, PIECE), jnp.float32),
        pltpu.VMEM((own // PIECE, late, PIECE), jnp.float32),
    ]
    high, sums, late_high, late_sums, *columns_near, kept_1, turned_1 = call(
        make_late_kernel(scale, False, rows),
        "late_near",
        (*row, *late_row, array(8, own), array(8, own), array(rows, late), array(rows, late)),
        early_q,
        late_q,
        early_p,
        late_p,
        high,
        sums,
        *columns_near,
        scratch=scores,
    )
    mine, kept_3 = call(
        make_late_kernel(scale, True, rows),
        "late_far",
        (array(5 * slots // 2, 128), array(rows, late)),
        early_q,
        late_q,
        early_far_p,
        late_far_p,
        high,
        sums,
        *columns_far,
        late_high,
        late_sums,
        *columns_near,
        scratch=scores,
    )
    theirs = exchanged(mine, core)
    all_q, all_p = (early_q, late_q, early_far_q, late_far_q), (early_p, late_p, early_far_p, late_far_p)
    (turned_2,) = call(make_scores_kernel(), "own_scores", (array(rows, own),), early_p, *all_q[2:])
    shape = jax.ShapeDtypeStruct((rows, half), jnp.float32)
    return call(
        make_gradient_kernel(slots, rows, half, scale),
        "gradients",
        (shape, shape),
        *all_q,
        *all_p,
        kept_0,
        kept_1,
        kept_2,
        kept_3,
        turned_0,
        turned_1,
        turned_2,
        keys,
        mine,
        theirs,
    )


def fits(rows, half, slots, across):
    everything = slots * rows
    if rows != 128 or half % 128 or across != 2 or slots % 4 or slots & (slots - 1):
        return False
    return everything * half * 16 + everything * everything * 2 <= VMEM_BYTES // 2


def local(queries, passages, positives):
    shape = (*queries.shape, lax.axis_size("batch"), lax.axis_size("rep"))
    if not fits(*shape):
        return streamed(queries, passages, positives)
    return resident(queries, passages, positives)


def solution(mesh):
    in_specs = (P("batch", "rep"), P("batch", "rep"), P())
    out_specs = (P("batch", "rep"), P("batch", "rep"))
    return jax.shard_map(local, mesh=mesh, in_specs=in_specs, out_specs=out_specs, check_vma=False)
```

```python
import math

import jax
import jax.numpy as jnp
from jax import lax
from jax.experimental import pallas as pl
from jax.experimental.pallas import tpu as pltpu
from jax.sharding import PartitionSpec as P


NEGATIVE = -1e30
LOG2E = 1.4426950408889634
VMEM_BYTES = 58 * 2**20
DIAGONAL = "xyxd"
PIECE = 256


def joined(x, axis, combine):
    everything = jax.tree.map(lambda part: lax.all_gather(part, axis), x)
    first = jax.tree.map(lambda part: part[0], everything)

    def turn(k, so_far):
        return combine(so_far, jax.tree.map(lambda part: part[k], everything))

    return lax.fori_loop(1, lax.axis_size(axis), turn, first)


def sweep_blocks(update, running, members, offset):
    piece_rows = members[0].shape[0]
    if piece_rows > 1024 and piece_rows % 512 == 0:

        def advance(carried, block_index):
            sliced = tuple(
                (lax.dynamic_slice_in_dim(member, block_index * 512, 512, 0) for member in members)
            )
            return (update(carried, sliced, offset + block_index * 512), None)

        running, _ = lax.scan(advance, running, jnp.arange(piece_rows // 512, dtype=jnp.int32))
        return running
    return update(running, members, offset)


def combine_pairs(former, latter):
    results = []
    for position in range(0, len(former), 2):
        highest = jnp.maximum(former[position], latter[position])
        summed = former[position + 1] * jnp.exp(former[position] - highest) + latter[
            position + 1
        ] * jnp.exp(latter[position] - highest)
        results.extend([highest, summed])
    return tuple(results)


def pair_scores(local_set, remote_set, logit_scale):
    products = lax.dot_general(
        local_set, remote_set, (((1,), (1,)), ((), ())), preferred_element_type=jnp.float32
    )
    return products * logit_scale


def weighted_sum(
    local_set, local_norm, local_keys, remote_set, remote_norm, remote_keys, logit_scale
):
    scores = pair_scores(local_set, remote_set, logit_scale)
    matches = (local_keys[:, None] == remote_keys[None, :]).astype(jnp.float32)
    weights = (
        jnp.exp(scores - local_norm[:, None])
        + jnp.exp(scores - remote_norm[None, :])
        - 2.0 * matches
    )
    return jnp.dot(weights.astype(jnp.bfloat16), remote_set, preferred_element_type=jnp.float32)


def streamed(queries, passages, positives):
    own_rows = queries.shape[0]
    half_rows = own_rows // 2
    model_width = queries.shape[1] * lax.axis_size("rep")
    batch_count = lax.axis_size("batch")
    all_rows = batch_count * own_rows
    column_count = batch_count * half_rows
    logit_scale = 1.0 / math.sqrt(model_width)
    batch_index = lax.axis_index("batch")
    rep_index = lax.axis_index("rep")
    block_start = batch_index * own_rows
    half_start = rep_index * half_rows
    query_full, passage_full = (
        lax.all_gather(queries, "rep", axis=1, tiled=True),
        lax.all_gather(passages, "rep", axis=1, tiled=True),
    )
    passage_half = lax.dynamic_slice_in_dim(passage_full, half_start, half_rows, 0)

    def score_update(running, sliced, offset):
        row_high, row_total, column_high, column_total = running
        scores = pair_scores(query_full, sliced[0], logit_scale)
        new_high = jnp.maximum(row_high, jnp.max(scores, axis=1))
        row_total = row_total * jnp.exp(row_high - new_high) + jnp.sum(
            jnp.exp(scores - new_high[:, None]), axis=1
        )
        piece_high = jnp.max(scores, axis=0)
        piece_total = jnp.sum(jnp.exp(scores - piece_high[None, :]), axis=0)
        column_high = lax.dynamic_update_slice_in_dim(column_high, piece_high, offset, 0)
        column_total = lax.dynamic_update_slice_in_dim(column_total, piece_total, offset, 0)
        return (new_high, row_total, column_high, column_total)

    starting = (
        jnp.full((own_rows,), NEGATIVE, jnp.float32),
        jnp.zeros((own_rows,), jnp.float32),
        jnp.full((column_count,), NEGATIVE, jnp.float32),
        jnp.zeros((column_count,), jnp.float32),
    )
    row_high, row_total, column_high, column_total = sweep_blocks(
        score_update,
        starting,
        (lax.all_gather(passage_half, "batch", axis=0, tiled=True),),
        jnp.int32(0),
    )
    row_high, row_total = joined((row_high, row_total), "rep", combine_pairs)
    column_high, column_total = joined((column_high, column_total), "batch", combine_pairs)
    row_norms = lax.all_gather(row_high + jnp.log(row_total), "batch", axis=0, tiled=True)
    column_halves = lax.all_gather(column_high + jnp.log(column_total), "rep", axis=0, tiled=True)
    column_norms = (
        column_halves.reshape(2, batch_count, half_rows).transpose(1, 0, 2).reshape(all_rows)
    )
    row_own = lax.dynamic_slice_in_dim(row_norms, block_start, own_rows, 0)
    column_own = lax.dynamic_slice_in_dim(column_norms, block_start, own_rows, 0)
    positive_own = lax.dynamic_slice_in_dim(positives, block_start, own_rows, 0)
    own_ids = block_start + jnp.arange(own_rows, dtype=jnp.int32)
    all_ids = jnp.arange(all_rows, dtype=jnp.int32)
    cleared = jnp.zeros((own_rows, model_width), jnp.float32)

    def half_order(vector):
        return lax.dynamic_slice_in_dim(
            vector.reshape(batch_count, own_rows), half_start, half_rows, 1
        ).reshape(column_count)

    column_order = half_order(column_norms)
    row_order = half_order(row_norms)
    positive_order = half_order(positives)
    passage_order = half_order(all_ids)
    query_half = lax.dynamic_slice_in_dim(query_full, half_start, half_rows, 0)

    def both_update(running, sliced, offset):
        query_sum, passage_sum = running
        passage_piece, query_piece = sliced
        piece_rows = passage_piece.shape[0]

        def window(vector):
            return lax.dynamic_slice_in_dim(vector, offset, piece_rows, 0)

        query_sum = query_sum + weighted_sum(
            query_full,
            row_own,
            positive_own,
            passage_piece,
            window(column_order),
            window(passage_order),
            logit_scale,
        )
        passage_sum = passage_sum + weighted_sum(
            passage_full,
            column_own,
            own_ids,
            query_piece,
            window(row_order),
            window(positive_order),
            logit_scale,
        )
        return (query_sum, passage_sum)

    query_sum, passage_sum = sweep_blocks(
        both_update,
        (cleared, cleared),
        (
            lax.all_gather(passage_half, "batch", axis=0, tiled=True),
            lax.all_gather(query_half, "batch", axis=0, tiled=True),
        ),
        jnp.int32(0),
    )
    grad_queries, grad_passages = (
        lax.psum_scatter(query_sum * logit_scale, "rep", scatter_dimension=1, tiled=True),
        lax.psum_scatter(passage_sum * logit_scale, "rep", scatter_dimension=1, tiled=True),
    )
    return (grad_queries, grad_passages)


def exchanged(x, bits):
    axes = ("batch", "rep")
    count = lax.axis_size("batch") * lax.axis_size("rep")
    return lax.ppermute(x, axes, [(i, i ^ bits) for i in range(count)])


def column_of(row):
    return jnp.broadcast_to(row, (128, 128)).T[:, :1]


def matmul(a, b, contract):
    return lax.dot_general(a, b, ((contract[:1], contract[1:]), ((), ())), preferred_element_type=jnp.float32)


def make_unit_kernel(offsets, rows):
    def kernel(index, queries, passages, positives, unit, keys, table, arrived):
        copies = [
            pltpu.make_async_copy(source, target, arrived.at[n])
            for n, (source, target) in enumerate(
                ((queries, unit.at[:rows]), (passages, unit.at[rows:]), (positives, table))
            )
        ]
        for copy in copies:
            copy.start()
        for copy in copies[::-1]:
            copy.wait()
        lane = lax.broadcasted_iota(jnp.int32, (1, rows), 1)
        for s, offset in enumerate(offsets):
            block = index[0] ^ offset
            keys[s : s + 1, :] = block * rows + lane
            keys[len(offsets) + s : len(offsets) + s + 1, :] = table[pl.ds(block, 1), :]

    return kernel


def make_pack_kernel(rows, half):
    def kernel(*refs):
        parts, query_out, passage_out = refs[:-2], refs[-2], refs[-1]
        count = len(parts) // 2
        for side in range(2):
            lanes = pl.ds(side * half, half)
            for s in range(count):
                query_out[pl.ds(s * rows, rows), lanes] = parts[side * count + s][:rows, :]
                passage_out[pl.ds(s * rows, rows), lanes] = parts[side * count + s][rows:, :]

    return kernel


def joined_stats(blocks, former, factor, fold):
    high = None if former is None else former[0]
    for block in blocks:
        for part in fold(block):
            high = part if high is None else jnp.maximum(high, part)
    sums = None if former is None else former[1] * jnp.exp2((former[0] - high) * factor)
    for block in blocks:
        for part in fold(block):
            more = jnp.exp2((part - high) * factor)
            sums = more if sums is None else sums + more
    return high, sums


def put_turned(out, block):
    for k in range(0, block.shape[0], 128):
        out[:, k : k + 128] = block[k : k + 128].T


def by_lane(block):
    return [block[:, k : k + 128] for k in range(0, block.shape[1], 128)]


def column_stats(blocks, former, factor):
    high = None if former is None else former[0]
    for block in blocks:
        peak = jnp.max(block[...].reshape(-1, 8, block.shape[1]), axis=0)
        high = peak if high is None else jnp.maximum(high, peak)
    sums = None if former is None else former[1] * jnp.exp2((former[0] - high) * factor)
    for block in blocks:
        part = jnp.sum(jnp.exp2((block[...].reshape(-1, 8, block.shape[1]) - high) * factor), axis=0)
        sums = part if sums is None else sums + part
    return high, sums


def make_early_kernel(factor, joins, rows):
    def kernel(*refs):
        queries, passages = refs[:2]
        high_out, sum_out, column_high, column_sum, kept = refs[-7:-2] if not joins else refs[-6:-1]
        scores = refs[-1]
        count = passages.shape[0] // PIECE
        blocks = [scores.at[j] for j in range(count)]
        for j in range(count):
            cut = slice(j * PIECE, (j + 1) * PIECE)
            s = matmul(queries[...], passages[cut, :], (1, 1))
            blocks[j][...] = s
            kept[:, cut] = s[:rows] * factor
            if j == 0 and not joins:
                put_turned(refs[-2], s[:, :rows] * factor)
            column_high[:, cut], column_sum[:, cut] = column_stats([blocks[j]], None, factor)
        former = (refs[2][...], refs[3][...]) if joins else None
        high_out[...], sum_out[...] = joined_stats(blocks, former, factor, by_lane)

    return kernel


def make_late_kernel(factor, last, rows):
    def kernel(*refs):
        early_q, late_q, early_p, late_p, high_in, sum_in, column_high, column_sum = refs[:8]
        across, corner = refs[-2:]
        kept = refs[-3 if last else -4]
        early, late = early_p.shape[0], late_p.shape[0]
        lead = (early + late) // 128
        pieces = late // PIECE
        tops = [across.at[j] for j in range(pieces)]
        corners = [corner.at[j] for j in range((early + late) // PIECE)]
        columns = []
        for j in range(early // PIECE):
            cut = slice(j * PIECE, (j + 1) * PIECE)
            block = corners[pieces + j]
            s = matmul(late_q[...], early_p[cut, :], (1, 1))
            block[...] = s
            if j == 0 and not last:
                put_turned(refs[-3], s[:, :rows] * factor)
            columns.append(column_stats([block], (column_high[:, cut], column_sum[:, cut]), factor))
        for j in range(pieces):
            cut = slice(j * PIECE, (j + 1) * PIECE)
            s = matmul(early_q[...], late_p[cut, :], (1, 1))
            tops[j][...] = s
            kept[:, cut] = s[:rows] * factor
            corners[j][...] = matmul(late_q[...], late_p[cut, :], (1, 1))
            columns.append(column_stats([tops[j], corners[j]], None, factor))
        late_former = (refs[8][...], refs[9][...]) if last else None
        groups = (
            joined_stats(tops, (high_in[...], sum_in[...]), factor, by_lane),
            joined_stats(corners, late_former, factor, by_lane),
        )
        if not last:
            for n, values in enumerate((*groups[0], *groups[1])):
                refs[8 + n][...] = values
            for j, (high, sums) in enumerate(columns):
                cut = slice(j * PIECE, (j + 1) * PIECE)
                refs[12][:, cut], refs[13][:, cut] = high, sums
            return
        out = refs[12]
        near = [(refs[10][:, j : j + PIECE], refs[11][:, j : j + PIECE]) for j in range(0, early + late, PIECE)]
        for side, pairs in enumerate((near, columns)):
            for j, (high, sums) in enumerate(pairs):
                top = jnp.max(high, axis=0, keepdims=True)
                total = jnp.sum(sums * jnp.exp2((high - top) * factor), axis=0, keepdims=True)
                for k in range(PIECE // 128):
                    cut, row = slice(k * 128, (k + 1) * 128), 2 * side * lead + j * (PIECE // 128) + k
                    out[row : row + 1, :] = top[:, cut] * factor
                    out[lead + row : lead + row + 1, :] = total[:, cut]
        row = 4 * lead
        first_half = lax.broadcasted_iota(jnp.int32, (128, 128), 1) < 64
        for high, sums in groups:
            top = jnp.max(high, axis=1, keepdims=True)
            total = jnp.sum(sums * jnp.exp2((high - top) * factor), axis=1, keepdims=True)
            for k in range(0, high.shape[0], 128):
                both = jnp.where(first_half, top[k : k + 128], total[k : k + 128]).T
                out[row : row + 1, :] = both[:1] * factor + jnp.log(both[64:65]) * LOG2E
                row += 1

    return kernel


def make_prepare_kernel(factor, slots, rows):
    near = slots // 2

    def kernel(own, early_far_q, late_far_q, *refs):
        kept, turned, mine, keys = refs[:4], refs[4:6], refs[6], refs[7]
        query_part, near_part, far_scores, far_match = refs[8:]
        end = 2 * slots
        norm = [mine[end + s : end + s + 1, :] for s in range(near)]
        row_own = column_of(norm[0])
        own_id, positive_own = (
            column_of(keys[s : s + 1, :].astype(jnp.float32)).astype(jnp.int32) for s in (0, slots)
        )
        start = 0
        for source in (early_far_q, late_far_q):
            for low in range(0, source.shape[0], PIECE):
                s = matmul(own[:rows, :], source[low : low + PIECE, :], (1, 1)) * factor
                far_scores[:, start : start + PIECE] = s
                start += PIECE
        slot = 0
        for n, part in enumerate((*kept, *turned)):
            for k in range(0, part.shape[1], rows):
                if n == len(kept) and k == 0:
                    slot = 0
                cut = slice(slot * rows, (slot + 1) * rows)
                s = part[:, k : k + rows]
                if n < len(kept):
                    match = jnp.where(positive_own == keys[slot : slot + 1, :], 2.0, 0.0)
                    query_part[:, cut] = jnp.exp2(s - row_own) - match
                else:
                    match = jnp.where(own_id == keys[slots + slot : slots + slot + 1, :], 2.0, 0.0)
                    near_part[:, cut] = jnp.exp2(s - norm[slot]) - match
                slot += 1
        for slot in range(near):
            row = slots + near + slot
            far_match[:, slot * rows : (slot + 1) * rows] = jnp.where(own_id == keys[row : row + 1, :], 2.0, 0.0)

    return kernel


def make_gradient_kernel(slots, rows, half, scale):
    near = slots // 2

    def kernel(*refs):
        queries, passages, kept, turned = refs[:4], refs[4:8], refs[8:12], refs[12:14]
        query_part, near_part, far_scores, far_match, mine, theirs, query_out, passage_out = refs[14:]
        column_norm = []
        for s in range(slots):
            c = s % near + s // near * slots
            t = (c + slots) % (2 * slots)
            high, high_far = mine[c : c + 1, :], theirs[t : t + 1, :]
            total, total_far = mine[c + near : c + near + 1, :], theirs[t + near : t + near + 1, :]
            top = jnp.maximum(high, high_far)
            summed = total * jnp.exp2(high - top) + total_far * jnp.exp2(high_far - top)
            column_norm.append(top + jnp.log(summed) * LOG2E)
        column_own = column_of(column_norm[0])
        row_far = [theirs[2 * slots + s : 2 * slots + s + 1, :] for s in range(near)]
        results = [None, None]
        spans = [(n, low) for n, source in enumerate(passages) for low in range(0, source.shape[0], PIECE)]
        for step, (n, low) in enumerate(spans):
            first, cut = step * PIECE // rows, slice(step * PIECE, (step + 1) * PIECE)
            norm = jnp.concatenate(column_norm[first : first + PIECE // rows], axis=1)
            weights = [query_part[:, cut] + jnp.exp2(kept[n][:, low : low + PIECE] - norm)]
            if first < near:
                weights.append(near_part[:, cut] + jnp.exp2(turned[n][:, low : low + PIECE] - column_own))
            else:
                cut = slice(step * PIECE - near * rows, (step + 1) * PIECE - near * rows)
                s = far_scores[:, cut]
                norm = jnp.concatenate(row_far[first - near : first - near + PIECE // rows], axis=1)
                weights.append(jnp.exp2(s - norm) + jnp.exp2(s - column_own) - far_match[:, cut])
            for k, everything in enumerate((passages, queries)):
                part = matmul(weights[k].astype(jnp.bfloat16), everything[n][low : low + PIECE, :half], (1, 0))
                results[k] = part if results[k] is None else results[k] + part
        query_out[...], passage_out[...] = results[0] * scale, results[1] * scale

    return kernel


def resident(queries, passages, positives):
    rows, half = queries.shape
    slots, across = lax.axis_size("batch"), lax.axis_size("rep")
    scale = 1.0 / math.sqrt(half * across)
    factor = scale * LOG2E
    core, near = across, 2 * across
    vmem = pl.BlockSpec(memory_space=pltpu.VMEM)

    def call(kernel, name, shapes, *args, scratch=()):
        specs = [pl.BlockSpec(memory_space=pltpu.SMEM) if a.size == 1 else vmem for a in args]
        if name == "unit":
            specs[1:] = [pl.BlockSpec(memory_space=pl.ANY)] * 3
        space = pltpu.HBM if name == "unit" else pltpu.VMEM
        args = [a if a.size == 1 else pltpu.with_memory_space_constraint(a, space) for a in args]
        return pl.pallas_call(
            kernel,
            out_shape=shapes,
            in_specs=specs,
            out_specs=tuple(vmem for _ in shapes),
            scratch_shapes=scratch,
            compiler_params=pltpu.CompilerParams(vmem_limit_bytes=VMEM_BYTES // 8),
        )(*args)

    def array(*shape, dtype=jnp.float32):
        return pltpu.VMEM(shape, dtype)

    late_slots = [s for s in range(slots // 2, slots, 2) if s & 2]
    early_slots = [s for s in range(0, slots, 2) if s not in late_slots]
    order = early_slots + late_slots
    order += [s ^ 1 for s in order]
    unit, keys = call(
        make_unit_kernel(order, rows),
        "unit",
        (array(2 * rows, half, dtype=queries.dtype), array(2 * slots, 128, dtype=jnp.int32)),
        lax.axis_index("batch")[None],
        queries,
        passages,
        positives.reshape(slots, rows),
        scratch=[pltpu.VMEM((slots, rows), jnp.int32), pltpu.SemaphoreType.DMA((3,))],
    )
    held = {0: unit}
    for k in range(4, slots, 4):
        source, bits = (held[k & (k - 1)], k & -k) if k & (k - 1) else (unit, k)
        held[k] = exchanged(source, bits * across)
    sides = [{}, {}]
    for k in range(0, slots, 4):
        n = k // 4
        sides[0][k] = held[k]
        sides[0][k + 2] = exchanged(held[k], near)
        sides[1][k] = exchanged(held[k], 1)
        mode = DIAGONAL[n % len(DIAGONAL)]
        if mode == "d":
            sides[1][k + 2] = exchanged(held[k], near + 1)
        elif mode == "x":
            sides[1][k + 2] = exchanged(sides[1][k], near)
        else:
            sides[1][k + 2] = exchanged(sides[0][k + 2], 1)

    def packed(name, chosen):
        shape = array(len(chosen) * rows, half * across, dtype=queries.dtype)
        parts = [side[s] for side in sides for s in chosen]
        q, p = call(make_pack_kernel(rows, half), "pack_" + name, (shape, shape), *parts)
        far_p, far_q = exchanged(p, core), exchanged(q, core)
        return q, p, far_q, far_p

    early, late = len(early_slots) * rows, len(late_slots) * rows
    early_q, early_p, early_far_q, early_far_p = packed("early", early_slots)
    own = slots // 2 * rows
    columns = (array(8, early), array(8, early))
    row = (array(early, 128), array(early, 128))
    scores = [pltpu.VMEM((early // PIECE, early, PIECE), jnp.float32)]
    high, sums, *columns_near, kept_0, turned_0 = call(
        make_early_kernel(factor, False, rows),
        "early_near",
        (*row, *columns, array(rows, early), array(rows, early)),
        early_q,
        early_p,
        scratch=scores,
    )
    high, sums, *columns_far, kept_2 = call(
        make_early_kernel(factor, True, rows),
        "early_far",
        (*row, *columns, array(rows, early)),
        early_q,
        early_far_p,
        high,
        sums,
        scratch=scores,
    )
    late_q, late_p, late_far_q, late_far_p = packed("late", late_slots)
    late_row = (array(late, 128), array(late, 128))
    scores = [
        pltpu.VMEM((late // PIECE, early, PIECE), jnp.float32),
        pltpu.VMEM((own // PIECE, late, PIECE), jnp.float32),
    ]
    high, sums, late_high, late_sums, *columns_near, kept_1, turned_1 = call(
        make_late_kernel(factor, False, rows),
        "late_near",
        (*row, *late_row, array(8, own), array(8, own), array(rows, late), array(rows, late)),
        early_q,
        late_q,
        early_p,
        late_p,
        high,
        sums,
        *columns_near,
        scratch=scores,
    )
    mine, kept_3 = call(
        make_late_kernel(factor, True, rows),
        "late_far",
        (array(5 * slots // 2, 128), array(rows, late)),
        early_q,
        late_q,
        early_far_p,
        late_far_p,
        high,
        sums,
        *columns_far,
        late_high,
        late_sums,
        *columns_near,
        scratch=scores,
    )
    theirs = exchanged(mine, core)
    all_q, all_p = (early_q, late_q, early_far_q, late_far_q), (early_p, late_p, early_far_p, late_far_p)
    kept, turned = (kept_0, kept_1, kept_2, kept_3), (turned_0, turned_1)
    prepared = call(
        make_prepare_kernel(factor, slots, rows),
        "prepare",
        (array(rows, slots * rows), *[array(rows, own)] * 3),
        early_p,
        *all_q[2:],
        *kept,
        *turned,
        mine,
        keys,
    )
    shape = jax.ShapeDtypeStruct((rows, half), jnp.float32)
    return call(
        make_gradient_kernel(slots, rows, half, scale),
        "gradients",
        (shape, shape),
        *all_q,
        *all_p,
        *kept,
        *turned,
        *prepared,
        mine,
        theirs,
    )


def fits(rows, half, slots, across):
    everything = slots * rows
    if rows != 128 or half % 128 or across != 2 or slots % 4 or slots & (slots - 1):
        return False
    return everything * half * 16 + everything * everything * 2 <= VMEM_BYTES // 2


def local(queries, passages, positives):
    shape = (*queries.shape, lax.axis_size("batch"), lax.axis_size("rep"))
    if not fits(*shape):
        return streamed(queries, passages, positives)
    return resident(queries, passages, positives)


def solution(mesh):
    in_specs = (P("batch", "rep"), P("batch", "rep"), P())
    out_specs = (P("batch", "rep"), P("batch", "rep"))
    return jax.shard_map(local, mesh=mesh, in_specs=in_specs, out_specs=out_specs, check_vma=False)
```
